32 devices in a mesh: samp: 8 (over z, x), feat: 4 (over y, core).
Axes of the slice: x: 2, y: 2, z: 4, core: 2. Of those that a mesh axis runs over, the one named last changes fastest.
Arguments:
- features: bfloat16 [131072, 2048], P('samp', 'feat'), may hold values from -40 to 40
- labels: int32 [131072], P('samp'), may hold values from 0 to 9
- weights: float32 [10, 2048], P(None, 'feat'), may hold values from -6 to 6
- sketch_basis: float32 [10, 2048, 512], P(None, 'feat'), may hold values from -0.0390625 to 0.0390625
- sketch_values: float32 [512], replicated, may hold values from 0.05 to 2
Outputs:
- newton_step: float32 [10, 2048], P(None, 'feat')
The draws below stay inside these ranges and needn't reach their ends.
All inputs are finite; a program needn't handle non-finite values.
Results may differ from the reference program's by a relative error of at most 0.001.
The reference program's roundings to bfloat16 on the way count: a program that leaves them out, or rounds other values in their place, can miss the bound.
Values may be sent and summed in bfloat16 or wider, within the bound.
A program may use at most 128 MiB of HBM per device.

```python
import math
import jax
import jax.numpy as jnp
from jax import lax

F = 2048
K = 10
R = 512
ITERS = 3
NS = 131072


def class_weights(key):
    drawn = jax.random.normal(jax.random.fold_in(key, 7001), (K, F), jnp.float32)
    return jnp.clip(drawn, -6.0, 6.0)


def draw_weights(key, part):
    return class_weights(key)


def draw_features(key, part):
    keys = jax.random.split(jax.random.fold_in(key, 7002), 4)
    columns = jnp.arange(F, dtype=jnp.float32)
    col_scale = jnp.exp(jax.random.uniform(keys[0], (F,), jnp.float32, math.log(0.5), math.log(5.0)))
    col_scale = col_scale * jnp.exp(0.5 * math.log(3.0) * columns / F)
    values = jax.random.normal(keys[3], (NS, F), jnp.float32) * col_scale[None, :]
    return jnp.clip(values, -40.0, 40.0).astype(jnp.bfloat16)


def set_ends(array, rng, least, top_value):
    longest = array.shape.index(max(array.shape))
    spots = []
    for shift in (0, 1):
        where = [jax.random.randint(jax.random.fold_in(rng, axis), (), 0, length) for axis, length in enumerate(array.shape)]
        where[longest] = (where[longest] + shift) % array.shape[longest]
        spots.append(tuple(where))
    return array.at[spots[0]].set(least).at[spots[1]].set(top_value)


def level_of(rng, dims, shards, least, largest):
    gain, own = 1.0, jax.random.fold_in(rng, 6)
    for axis_at, parts in shards:
        steps = jnp.exp(jax.random.uniform(jax.random.fold_in(own, axis_at), (parts,), jnp.float32, least / len(shards), largest / len(shards)))
        gain = gain * jnp.repeat(steps, dims[axis_at] // parts).reshape([-1 if axis == axis_at else 1 for axis in range(len(dims))])
    return gain


def gaussian(key, shape, spread, bound, shards=(), kind=jnp.bfloat16):
    loudness = level_of(key, shape, shards, -0.22, 0.18) if shards else 1.0
    entries = jax.random.normal(key, shape, jnp.float32) * spread * loudness
    return jnp.minimum(jnp.maximum(entries, -bound), bound).astype(kind)


def setup_inputs(seed: int = 0) -> dict:
    arg_keys = jax.random.split(jax.random.key(seed), 6)
    return {
        "features": draw_features(jax.random.fold_in(arg_keys[5], 71), 0),
        "labels": set_ends(jax.random.randint(arg_keys[1], (NS,), 0, K), jax.random.fold_in(arg_keys[1], 1), 0, K - 1).astype(jnp.int32),
        "weights": draw_weights(jax.random.fold_in(arg_keys[5], 71), 0),
        "sketch_basis": gaussian(arg_keys[3], (K, F, R), (F * K) ** -0.5, 0.0390625, ((1, 4),), jnp.float32),
        "sketch_values": jnp.clip(jnp.exp(jax.random.uniform(arg_keys[4], (R,), jnp.float32, math.log(0.05), math.log(2.0))), 0.05, 2.0),
    }


ridge = 0.05
contract_last = (((1,), (1,)), ((), ()))

def column_softmax(scores):
    column_max = lax.optimization_barrier(jnp.max(scores, axis=0, keepdims=True))
    shifted_exp = jnp.exp(scores - column_max)
    return shifted_exp / lax.optimization_barrier(jnp.sum(shifted_exp, axis=0, keepdims=True))

def reference(features, labels, weights, sketch_basis, sketch_values):
    total_rows = features.shape[0]

    def project(vector):
        return lax.dot_general(vector.astype(jnp.bfloat16).astype(jnp.float32), features.astype(jnp.float32), contract_last, preferred_element_type=jnp.float32)

    def collect(coeffs):
        return jnp.dot(coeffs.astype(jnp.bfloat16).astype(jnp.float32), features.astype(jnp.float32), preferred_element_type=jnp.float32)
    probabilities = column_softmax(project(weights) / math.sqrt(F))
    onehot = (labels[None, :] == jnp.arange(K, dtype=jnp.int32)[:, None]).astype(jnp.float32)
    gradient = collect(probabilities - onehot) * (math.sqrt(F) / total_rows) + ridge * weights

    def hessian(direction):
        image_vals = project(direction)
        weighted = probabilities * image_vals
        curvature = weighted - probabilities * lax.optimization_barrier(jnp.sum(weighted, axis=0, keepdims=True))
        return collect(curvature) / total_rows + ridge * direction
    flat_basis = sketch_basis.reshape(K * F, R)
    gram_matrix = jnp.dot(flat_basis.T, flat_basis, precision=lax.Precision.HIGHEST)
    factor = jnp.linalg.cholesky(gram_matrix)
    coefficients = (jnp.min(sketch_values) + ridge) / (sketch_values + ridge) - 1.0

    def precondition(residue):
        projection = jnp.dot(residue.reshape(-1), flat_basis, precision=lax.Precision.HIGHEST)
        inner_coords = jax.scipy.linalg.solve_triangular(factor, projection, lower=True)
        outer_coords = jax.scipy.linalg.solve_triangular(factor, coefficients * inner_coords, lower=True, trans=1)
        return residue + jnp.dot(flat_basis, outer_coords, precision=lax.Precision.HIGHEST).reshape(residue.shape)
    residue = -gradient
    newton_step = jnp.zeros_like(residue)
    scaled_res = precondition(residue)
    direction = scaled_res
    res_dot = jnp.sum(residue * scaled_res)
    for iteration in range(ITERS):
        hess_image = hessian(direction)
        step_size = res_dot / jnp.sum(direction * hess_image)
        newton_step = newton_step + step_size * direction
        if iteration + 1 < ITERS:
            residue = residue - step_size * hess_image
            scaled_res = precondition(residue)
            new_dot = jnp.sum(residue * scaled_res)
            direction = scaled_res + new_dot / res_dot * direction
            res_dot = new_dot
    return newton_step
```

```python
import functools
import math

import jax
import jax.numpy as jnp
from jax import lax
from jax.experimental import pallas as pl
from jax.experimental.pallas import tpu as pltpu
from jax.sharding import PartitionSpec as P

ITERS = 3


ridge = 0.05
contract_last = (((1,), (1,)), ((), ()))
contract_first = (((0,), (0,)), ((), ()))
MESH = pl.DeviceIdType.MESH
HIGHEST = lax.Precision.HIGHEST


def column_softmax(scores):
    column_max = jnp.max(scores, axis=0, keepdims=True)
    shifted_exp = jnp.exp(scores - column_max)
    return shifted_exp / jnp.sum(shifted_exp, axis=0, keepdims=True)


def product_kernel(first, nf, ns, scale, tile, *refs):
    if first:
        (feat_ref, vec_ref, lab_ref, out_ref, prob_ref,
         fbuf, part, got, coef, sums, load_sem,
         s1, r1, s2, r2, s3, r3) = refs
    else:
        (feat_ref, vec_ref, prob_ref, out_ref,
         fbuf, part, got, coef, sums, load_sem,
         s1, r1, s2, r2, s3, r3) = refs
    me = lax.axis_index("feat")
    row = lax.axis_index("samp")
    classes = vec_ref.shape[0]
    share = fbuf.shape[1]
    order = sorted(range(1, nf), key=lambda s: -min(s, nf - s)) + [0]

    loads = {}
    for s in order:
        q = lax.rem(me + s, nf)
        loads[s] = pltpu.make_async_copy(
            feat_ref.at[pl.ds(pl.multiple_of(q * share, share), share), :],
            fbuf.at[s], load_sem.at[s])
        loads[s].start()
    barrier = pltpu.get_barrier_semaphore()
    for s in range(1, nf):
        pl.semaphore_signal(barrier, inc=1, device_id={"feat": lax.rem(me + s, nf)}, device_id_type=MESH)
    for s in range(1, ns):
        pl.semaphore_signal(barrier, inc=1, device_id={"samp": lax.rem(row + s, ns)}, device_id_type=MESH)

    vec = vec_ref[...]
    sends = []
    for at, s in enumerate(order):
        loads[s].wait()

        @pl.loop(0, share // tile)
        def _(i, s=s):
            rows = pl.ds(pl.multiple_of(i * tile, tile), tile)
            part[s, :, rows] = lax.dot_general(
                vec, fbuf[s, rows, :], contract_last, preferred_element_type=jnp.float32)
        if at == 0:
            pl.semaphore_wait(barrier, nf - 1 + ns - 1)
        if s:
            copy = pltpu.make_async_remote_copy(
                src_ref=part.at[s], dst_ref=got.at[s - 1],
                send_sem=s1.at[s - 1], recv_sem=r1.at[s - 1],
                device_id={"feat": lax.rem(me + s, nf)}, device_id_type=MESH)
            copy.start()
            sends.append(copy)
    for copy in sends:
        copy.wait_recv()

    @pl.loop(0, share // tile)
    def _(i):
        rows = pl.ds(pl.multiple_of(i * tile, tile), tile)
        scores = part[0, :, rows]
        for s in range(nf - 1):
            scores = scores + got[s, :, rows]
        if first:
            prob = column_softmax(scores * scale)
            prob_ref[:, rows] = prob
            hot = lab_ref[:, rows] == lax.broadcasted_iota(jnp.int32, (classes, tile), 0)
            coef[0, :, rows] = (prob - hot.astype(jnp.float32)).astype(jnp.bfloat16)
        else:
            prob = prob_ref[:, rows]
            weighted = prob * scores
            coef[0, :, rows] = (
                weighted - prob * jnp.sum(weighted, axis=0, keepdims=True)).astype(jnp.bfloat16)

    gathers = {}
    for s in order[:-1]:
        copy = pltpu.make_async_remote_copy(
            src_ref=coef.at[0], dst_ref=coef.at[nf - s],
            send_sem=s2.at[s - 1], recv_sem=r2.at[nf - s - 1],
            device_id={"feat": lax.rem(me + s, nf)}, device_id_type=MESH)
        copy.start()
        gathers[s] = copy
    near = [s for s in reversed(order)]
    sums[0] = jnp.zeros(sums.shape[1:], jnp.float32)
    for s in near:
        if s:
            gathers[nf - s].wait_recv()

        @pl.loop(0, share // tile)
        def _(i, s=s):
            rows = pl.ds(pl.multiple_of(i * tile, tile), tile)
            sums[0] += jnp.dot(coef[s, :, rows], fbuf[s, rows, :], preferred_element_type=jnp.float32)
    totals = []
    for s in sorted(range(1, ns), key=lambda s: -min(s, ns - s)):
        copy = pltpu.make_async_remote_copy(
            src_ref=sums.at[0], dst_ref=sums.at[s],
            send_sem=s3.at[s - 1], recv_sem=r3.at[s - 1],
            device_id={"samp": lax.rem(row + s, ns)}, device_id_type=MESH)
        copy.start()
        totals.append(copy)
    for copy in totals:
        copy.wait_recv()
    total = sums[lax.rem(row, ns)]
    for t in range(1, ns):
        total = total + sums[lax.rem(row + ns - t, ns)]
    out_ref[...] = total
    for copy in sends + list(gathers.values()) + totals:
        copy.wait_send()


def sample_product(first, features, vector, side, nf, ns, scale):
    classes, cols = vector.shape
    local_rows = features.shape[0]
    share = local_rows // nf
    tile = min(1024, share)
    out_shape = [jax.ShapeDtypeStruct((classes, cols), jnp.float32)]
    if first:
        out_shape.append(jax.ShapeDtypeStruct((classes, share), jnp.float32))
    vmem = pl.BlockSpec(memory_space=pltpu.VMEM)
    dma = pltpu.SemaphoreType.DMA
    return pl.pallas_call(
        functools.partial(product_kernel, first, nf, ns, scale, tile),
        out_shape=out_shape,
        in_specs=[pl.BlockSpec(memory_space=pl.ANY), vmem, vmem],
        out_specs=[vmem] * len(out_shape),
        scratch_shapes=[
            pltpu.VMEM((nf, share, cols), jnp.bfloat16),
            pltpu.VMEM((nf, classes, share), jnp.float32),
            pltpu.VMEM((nf - 1, classes, share), jnp.float32),
            pltpu.VMEM((nf, classes, share), jnp.bfloat16),
            pltpu.VMEM((ns, classes, cols), jnp.float32),
            dma((nf,)),
            dma((nf - 1,)), dma((nf - 1,)),
            dma((nf - 1,)), dma((nf - 1,)),
            dma((ns - 1,)), dma((ns - 1,)),
        ],
        compiler_params=pltpu.CompilerParams(
            collective_id=0 if first else 1, has_side_effects=True,
            vmem_limit_bytes=48 * 1024 * 1024),
        cost_estimate=pl.CostEstimate(
            flops=4 * classes * local_rows * cols, bytes_accessed=2 * local_rows * cols, transcendentals=0),
        name="first_product" if first else "curvature_product",
    )(features, vector, side)


def on_device(features, labels, weights, sketch_basis, sketch_values):
    classes, local_cols = weights.shape
    local_rows = features.shape[0]
    sketch_rank = sketch_basis.shape[2]
    ns, nf = lax.axis_size("samp"), lax.axis_size("feat")
    total_rows = local_rows * ns
    total_cols = local_cols * nf
    share = local_rows // nf

    flat_local = sketch_basis.reshape(classes * local_cols, sketch_rank)
    local_gram = lax.dot_general(flat_local, flat_local, contract_first, precision=HIGHEST)
    gram_matrix = lax.psum(local_gram, "feat")

    own_labels = lax.dynamic_slice(labels, (lax.axis_index("feat") * share,), (share,))[None, :]
    sums, probabilities = sample_product(
        True, features, weights.astype(jnp.bfloat16), own_labels, nf, ns, 1.0 / math.sqrt(total_cols))
    gradient = sums * (math.sqrt(total_cols) / total_rows) + ridge * weights

    factor = jnp.linalg.cholesky(gram_matrix)
    coefficients = (jnp.min(sketch_values) + ridge) / (sketch_values + ridge) - 1.0
    inverse = jax.scipy.linalg.solve_triangular(
        factor, jnp.eye(sketch_rank, dtype=jnp.float32), lower=True)

    def precondition(residue):
        local_proj = jnp.dot(residue.reshape(-1), flat_local, precision=HIGHEST)
        both = lax.psum(jnp.concatenate([local_proj, jnp.sum(residue * residue)[None]]), "feat")
        inner = jnp.sum(inverse * both[None, :sketch_rank], axis=1)
        outer = jnp.sum(inverse * (coefficients * inner)[:, None], axis=0)
        scaled = residue + jnp.dot(flat_local, outer, precision=HIGHEST).reshape(residue.shape)
        return scaled, both[sketch_rank] + jnp.sum(coefficients * inner * inner)

    residue = -gradient
    newton_part = jnp.zeros_like(residue)
    scaled_res, res_dot = precondition(residue)
    direction = scaled_res
    for iteration in range(ITERS):
        (sums,) = sample_product(
            False, features, direction.astype(jnp.bfloat16), probabilities, nf, ns, 1.0)
        hess_image = sums / total_rows + ridge * direction
        step_size = res_dot / lax.psum(jnp.sum(direction * hess_image), "feat")
        newton_part = newton_part + step_size * direction
        if iteration + 1 < ITERS:
            residue = residue - step_size * hess_image
            scaled_res, new_dot = precondition(residue)
            direction = scaled_res + new_dot / res_dot * direction
            res_dot = new_dot
    return newton_part


def solution(mesh):
    in_specs = (P("samp", "feat"), P("samp"), P(None, "feat"), P(None, "feat", None), P())
    out_specs = P(None, "feat")
    return jax.shard_map(
        on_device, mesh=mesh, in_specs=in_specs, out_specs=out_specs, check_vma=False
    )
```

```python
import functools
import math

import jax
import jax.numpy as jnp
from jax import lax
from jax.experimental import pallas as pl
from jax.experimental.pallas import tpu as pltpu
from jax.sharding import PartitionSpec as P

ITERS = 3


ridge = 0.05
contract_last = (((1,), (1,)), ((), ()))
contract_first = (((0,), (0,)), ((), ()))
MESH = pl.DeviceIdType.MESH
HIGHEST = lax.Precision.HIGHEST


def column_softmax(scores):
    column_max = jnp.max(scores, axis=0, keepdims=True)
    shifted_exp = jnp.exp(scores - column_max)
    return shifted_exp / jnp.sum(shifted_exp, axis=0, keepdims=True)


def product_kernel(first, nf, ns, scale, tile, *refs):
    if first:
        (feat_ref, vec_ref, lab_ref, out_ref, prob_ref,
         fbuf, part, got, coef, sums, load_sem,
         s1, r1, s2, r2, s3, r3) = refs
    else:
        (feat_ref, vec_ref, prob_ref, out_ref,
         fbuf, part, got, coef, sums, load_sem,
         s1, r1, s2, r2, s3, r3) = refs
    me = lax.axis_index("feat")
    row = lax.axis_index("samp")
    classes = vec_ref.shape[0]
    share = fbuf.shape[1]
    order = sorted(range(1, nf), key=lambda s: -min(s, nf - s)) + [0]

    loads = {}
    for s in order:
        q = lax.rem(me + s, nf)
        loads[s] = pltpu.make_async_copy(
            feat_ref.at[pl.ds(pl.multiple_of(q * share, share), share), :],
            fbuf.at[s], load_sem.at[s])
        loads[s].start()
    barrier = pltpu.get_barrier_semaphore()
    for s in range(1, nf):
        pl.semaphore_signal(barrier, inc=1, device_id={"feat": lax.rem(me + s, nf)}, device_id_type=MESH)
    for s in range(1, ns):
        pl.semaphore_signal(barrier, inc=1, device_id={"samp": lax.rem(row + s, ns)}, device_id_type=MESH)

    vec = vec_ref[...]
    sends = []
    for at, s in enumerate(order):
        loads[s].wait()

        @pl.loop(0, share // tile)
        def _(i, s=s):
            rows = pl.ds(pl.multiple_of(i * tile, tile), tile)
            part[s, :, rows] = lax.dot_general(
                vec, fbuf[s, rows, :], contract_last, preferred_element_type=jnp.float32)
        if at == 0:
            pl.semaphore_wait(barrier, nf - 1 + ns - 1)
        if s:
            copy = pltpu.make_async_remote_copy(
                src_ref=part.at[s], dst_ref=got.at[s - 1],
                send_sem=s1.at[s - 1], recv_sem=r1.at[s - 1],
                device_id={"feat": lax.rem(me + s, nf)}, device_id_type=MESH)
            copy.start()
            sends.append(copy)
    for copy in sends:
        copy.wait_recv()

    @pl.loop(0, share // tile)
    def _(i):
        rows = pl.ds(pl.multiple_of(i * tile, tile), tile)
        scores = part[0, :, rows]
        for s in range(nf - 1):
            scores = scores + got[s, :, rows]
        if first:
            prob = column_softmax(scores * scale)
            prob_ref[:, rows] = prob
            hot = lab_ref[:, rows] == lax.broadcasted_iota(jnp.int32, (classes, tile), 0)
            coef[0, :, rows] = (prob - hot.astype(jnp.float32)).astype(jnp.bfloat16)
        else:
            prob = prob_ref[:, rows]
            weighted = prob * scores
            coef[0, :, rows] = (
                weighted - prob * jnp.sum(weighted, axis=0, keepdims=True)).astype(jnp.bfloat16)

    gathers = {}
    for s in order[:-1]:
        copy = pltpu.make_async_remote_copy(
            src_ref=coef.at[0], dst_ref=coef.at[nf - s],
            send_sem=s2.at[s - 1], recv_sem=r2.at[nf - s - 1],
            device_id={"feat": lax.rem(me + s, nf)}, device_id_type=MESH)
        copy.start()
        gathers[s] = copy
    near = [s for s in reversed(order)]
    sums[0] = jnp.zeros(sums.shape[1:], jnp.float32)
    for s in near:
        if s:
            gathers[nf - s].wait_recv()

        @pl.loop(0, share // tile)
        def _(i, s=s):
            rows = pl.ds(pl.multiple_of(i * tile, tile), tile)
            sums[0] += jnp.dot(coef[s, :, rows], fbuf[s, rows, :], preferred_element_type=jnp.float32)
    totals = []
    for s in sorted(range(1, ns), key=lambda s: -min(s, ns - s)):
        copy = pltpu.make_async_remote_copy(
            src_ref=sums.at[0], dst_ref=sums.at[s],
            send_sem=s3.at[s - 1], recv_sem=r3.at[s - 1],
            device_id={"samp": lax.rem(row + s, ns)}, device_id_type=MESH)
        copy.start()
        totals.append(copy)
    for copy in totals:
        copy.wait_recv()
    total = sums[lax.rem(row, ns)]
    for t in range(1, ns):
        total = total + sums[lax.rem(row + ns - t, ns)]
    out_ref[...] = total
    for copy in sends + list(gathers.values()) + totals:
        copy.wait_send()


def sample_product(first, features, vector, side, nf, ns, scale):
    classes, cols = vector.shape
    local_rows = features.shape[0]
    share = local_rows // nf
    tile = min(1024, share)
    out_shape = [jax.ShapeDtypeStruct((classes, cols), jnp.float32)]
    if first:
        out_shape.append(jax.ShapeDtypeStruct((classes, share), jnp.float32))
    vmem = pl.BlockSpec(memory_space=pltpu.VMEM)
    dma = pltpu.SemaphoreType.DMA
    return pl.pallas_call(
        functools.partial(product_kernel, first, nf, ns, scale, tile),
        out_shape=out_shape,
        in_specs=[pl.BlockSpec(memory_space=pl.ANY), vmem, vmem],
        out_specs=[vmem] * len(out_shape),
        scratch_shapes=[
            pltpu.VMEM((nf, share, cols), jnp.bfloat16),
            pltpu.VMEM((nf, classes, share), jnp.float32),
            pltpu.VMEM((nf - 1, classes, share), jnp.float32),
            pltpu.VMEM((nf, classes, share), jnp.bfloat16),
            pltpu.VMEM((ns, classes, cols), jnp.float32),
            dma((nf,)),
            dma((nf - 1,)), dma((nf - 1,)),
            dma((nf - 1,)), dma((nf - 1,)),
            dma((ns - 1,)), dma((ns - 1,)),
        ],
        compiler_params=pltpu.CompilerParams(
            collective_id=0 if first else 1, has_side_effects=True,
            vmem_limit_bytes=48 * 1024 * 1024),
        cost_estimate=pl.CostEstimate(
            flops=4 * classes * local_rows * cols, bytes_accessed=2 * local_rows * cols, transcendentals=0),
        name="first_product" if first else "curvature_product",
    )(features, vector, side)


def inverse_factor_kernel(block, gram_ref, out_ref, work, low, tri):
    size = gram_ref.shape[0]
    rowid = lax.broadcasted_iota(jnp.int32, (block, block), 0)
    lane = lax.broadcasted_iota(jnp.int32, (block, block), 1)
    work[...] = gram_ref[...]
    out_ref[...] = jnp.zeros_like(out_ref)
    for at in range(0, size, block):
        end = at + block
        tri[...] = work[at:end, at:end]

        @pl.loop(0, block)
        def _(t):
            held = tri[...]
            row = tri[pl.ds(t, 1), :]
            column = jnp.sum(jnp.where(lane == t, held, 0.0), axis=1, keepdims=True)
            pivot = jnp.sum(jnp.where(lane[:1] == t, row, 0.0), axis=1, keepdims=True)
            row = jnp.where(lane[:1] == t, 1.0, row) * (1.0 / pivot)
            below = jnp.where(lane == t, 0.0, held) - column * row
            tri[...] = jnp.where(rowid > t, below, held)

        held = tri[...]
        pivots = jnp.sum(jnp.where(lane == rowid, held, 0.0), axis=1, keepdims=True)
        unit = jnp.where(lane < rowid, held, jnp.where(lane == rowid, 1.0, 0.0))
        own = unit * (1.0 / jnp.sqrt(pivots))
        out_ref[at:end, at:end] = own
        if at:
            inner = jnp.dot(low[at:end, :at], out_ref[:at, :at], precision=HIGHEST,
                            preferred_element_type=jnp.float32)
            out_ref[at:end, :at] = -jnp.dot(own, inner, precision=HIGHEST,
                                            preferred_element_type=jnp.float32)
        if end < size:
            panel = lax.dot_general(work[end:, at:end], own, contract_last, precision=HIGHEST,
                                    preferred_element_type=jnp.float32)
            low[end:, at:end] = panel
            work[end:, end:] -= lax.dot_general(panel, panel, contract_last, precision=HIGHEST,
                                                preferred_element_type=jnp.float32)


def inverse_factor(gram_matrix):
    size = gram_matrix.shape[0]
    block = math.gcd(size, 128)
    vmem = pl.BlockSpec(memory_space=pltpu.VMEM)
    return pl.pallas_call(
        functools.partial(inverse_factor_kernel, block),
        out_shape=jax.ShapeDtypeStruct((size, size), jnp.float32),
        in_specs=[vmem],
        out_specs=vmem,
        scratch_shapes=[pltpu.VMEM((size, size), jnp.float32)] * 2 + [pltpu.VMEM((block, block), jnp.float32)],
        compiler_params=pltpu.CompilerParams(vmem_limit_bytes=16 * 1024 * 1024),
        cost_estimate=pl.CostEstimate(flops=12 * size ** 3, bytes_accessed=8 * size * size, transcendentals=0),
        name="inverse_factor",
    )(gram_matrix)


def on_device(features, labels, weights, sketch_basis, sketch_values):
    classes, local_cols = weights.shape
    local_rows = features.shape[0]
    sketch_rank = sketch_basis.shape[2]
    ns, nf = lax.axis_size("samp"), lax.axis_size("feat")
    total_rows = local_rows * ns
    total_cols = local_cols * nf
    share = local_rows // nf

    flat_local = sketch_basis.reshape(classes * local_cols, sketch_rank)
    local_gram = lax.dot_general(flat_local, flat_local, contract_first, precision=lax.Precision.HIGH)
    gram_matrix = lax.psum(local_gram, "feat")

    own_labels = lax.dynamic_slice(labels, (lax.axis_index("feat") * share,), (share,))[None, :]
    sums, probabilities = sample_product(
        True, features, weights.astype(jnp.bfloat16), own_labels, nf, ns, 1.0 / math.sqrt(total_cols))
    gradient = sums * (math.sqrt(total_cols) / total_rows) + ridge * weights

    coefficients = (jnp.min(sketch_values) + ridge) / (sketch_values + ridge) - 1.0
    inverse = inverse_factor(gram_matrix)

    def precondition(residue):
        local_proj = jnp.dot(residue.reshape(-1), flat_local, precision=HIGHEST)
        both = lax.psum(jnp.concatenate([local_proj, jnp.sum(residue * residue)[None]]), "feat")
        inner = jnp.sum(inverse * both[None, :sketch_rank], axis=1)
        outer = jnp.sum(inverse * (coefficients * inner)[:, None], axis=0)
        scaled = residue + jnp.sum(flat_local * outer[None, :], axis=1).reshape(residue.shape)
        return scaled, both[sketch_rank] + jnp.sum(coefficients * inner * inner)

    residue = -gradient
    newton_part = jnp.zeros_like(residue)
    scaled_res, res_dot = precondition(residue)
    direction = scaled_res
    for iteration in range(ITERS):
        (sums,) = sample_product(
            False, features, direction.astype(jnp.bfloat16), probabilities, nf, ns, 1.0)
        hess_image = sums / total_rows + ridge * direction
        step_size = res_dot / lax.psum(jnp.sum(direction * hess_image), "feat")
        newton_part = newton_part + step_size * direction
        if iteration + 1 < ITERS:
            residue = residue - step_size * hess_image
            scaled_res, new_dot = precondition(residue)
            direction = scaled_res + new_dot / res_dot * direction
            res_dot = new_dot
    return newton_part


def solution(mesh):
    in_specs = (P("samp", "feat"), P("samp"), P(None, "feat"), P(None, "feat", None), P())
    out_specs = P(None, "feat")
    return jax.shard_map(
        on_device, mesh=mesh, in_specs=in_specs, out_specs=out_specs, check_vma=False
    )
```
